256 devices in a mesh: macro: 128 (over y, x_lo, z, core), micro: 2 (over x_hi).
Axes of the slice: x: 4 (x_hi: 2, x_lo: 2; x = x_hi * 2 + x_lo), y: 4, z: 8, core: 2. Of those that a mesh axis runs over, the one named last changes fastest.
Arguments:
- macro_state: float32 [65536, 128], P('macro'), may hold values from -6 to 6
- micro_state: bfloat16 [65536, 12, 512], P('macro', None, 'micro'), may hold values from -6 to 6
- velocity: float32 [65536], P('macro'), may hold values from 0.25 to 4
- propagator: bfloat16 [512, 512], P(None, 'micro'), may hold values from -1 to 1
- forcing_map: float32 [128, 512], P(None, 'micro'), may hold values from -0.5 to 0.5
- readout: float32 [128, 512], P(None, 'micro'), may hold values from -1 to 1
- speed_weights: float32 [128], replicated, may hold values from -0.5 to 0.5
Outputs:
- macro_next: float32 [65536, 128], P('macro')
- micro_final: bfloat16 [65536, 12, 512], P('macro', None, 'micro')
The draws below stay inside these ranges and needn't reach their ends.
All inputs are finite; a program needn't handle non-finite values.
Results may differ from the reference program's by a relative error of at most 0.006.
Values may be sent and summed in bfloat16 or wider, within the bound.
No kernel may reach another device: no remote copies, remote signals or barrier semaphores. Data moves between devices by JAX's collectives and lax.ppermute only.
A program may use at most 64 MiB of HBM per device.

```python
import jax
import jax.numpy as jnp
from jax import lax

P_DEV = 512
S = 12
F = 512
NC = 128
STEPS = 4
M = 65536
N_MACRO = 128


def draw_velocity(key, part):
    base_key = jax.random.fold_in(key, 11)
    spot_key = jax.random.fold_in(key, 12)
    base = jnp.exp(jax.random.uniform(base_key, (M,), jnp.float32, jnp.log(0.25), 0.0))
    spot = jax.random.randint(spot_key, (), 0, M)
    places = jnp.arange(M)
    return jnp.where(places == spot, 4.0, base).astype(jnp.float32)


def draw_propagator(key, part):
    diag_key = jax.random.fold_in(key, 21)
    off_key = jax.random.fold_in(key, 22)
    diagonal = jax.random.uniform(diag_key, (F,), jnp.float32, 0.05, 0.95)
    offdiag = jnp.clip(jax.random.normal(off_key, (F, F), jnp.float32), -6.0, 6.0) * 0.3 / F ** 0.5
    offdiag = offdiag * (1.0 - jnp.eye(F, dtype=jnp.float32))
    return (offdiag + jnp.diag(diagonal)).astype(jnp.bfloat16)


def block_scale(rng, shape, split, low, high):
    loudness = 1.0
    for position, parts in split:
        draws = jax.random.uniform(jax.random.fold_in(jax.random.fold_in(rng, 6), position), (parts,), jnp.float32, low / len(split), high / len(split))
        loudness = loudness * jnp.repeat(jnp.exp(draws), shape[position] // parts).reshape((-1,) + (1,) * (len(shape) - 1 - position))
    return loudness


def normal_values(stream_key, shape, scale, bound, shards=(), kind=jnp.bfloat16):
    level = block_scale(stream_key, shape, shards, -0.22, 0.18) if shards else 1.0
    values = jax.random.normal(stream_key, shape, jnp.float32) * scale * level
    return jnp.minimum(jnp.maximum(values, -bound), bound).astype(kind)


def setup_inputs(seed: int = 0) -> dict:
    key_list = jax.random.split(jax.random.key(seed), 8)
    macro_state = normal_values(key_list[0], (M, NC), 1.0, 6.0, ((0, 128),), jnp.float32)
    micro_state = normal_values(key_list[1], (M, S, F), 1.0, 6.0, ((0, 128), (2, 2)))
    velocity = draw_velocity(jax.random.fold_in(key_list[7], 71), 0)
    propagator = draw_propagator(jax.random.fold_in(key_list[7], 71), 0)
    forcing_map = normal_values(key_list[4], (NC, F), NC ** -0.5, 0.5, ((1, 2),), jnp.float32)
    readout = normal_values(key_list[5], (NC, F), (F // 16) ** -0.5, 1.0, ((1, 2),), jnp.float32)
    speed_weights = normal_values(key_list[6], (NC,), NC ** -0.5, 0.5, (), jnp.float32)
    return {"macro_state": macro_state, "micro_state": micro_state, "velocity": velocity, "propagator": propagator, "forcing_map": forcing_map, "readout": readout, "speed_weights": speed_weights}


def reference(macro_state, micro_state, velocity, propagator, forcing_map, readout, speed_weights):
    highest = lax.Precision.HIGHEST
    forcing = jnp.tanh(jnp.dot(macro_state, forcing_map, precision=highest, preferred_element_type=jnp.float32))
    coupling = propagator.astype(jnp.float32)

    def advance(inputs):
        states, drive_rows = inputs
        tanh_sum = jnp.zeros(drive_rows.shape, jnp.float32)
        for _ in range(STEPS):
            mixed = jnp.einsum("psf,fg->psg", states.astype(jnp.float32), coupling, precision=highest)
            states = (mixed + drive_rows[:, None, :]).astype(jnp.bfloat16)
            tanh_sum = tanh_sum + jnp.sum(jnp.tanh(states.astype(jnp.float32)), axis=1)
        return states, tanh_sum

    blocks = (micro_state.reshape(N_MACRO, P_DEV, S, F), forcing.reshape(N_MACRO, P_DEV, F))
    final_states, tanh_sums = lax.map(advance, blocks)
    micro_final = final_states.reshape(M, S, F)
    averaged = tanh_sums.reshape(M, F) / (STEPS * S)
    forces = jnp.dot(averaged, readout.T, precision=highest, preferred_element_type=jnp.float32)
    drive_in = jnp.dot(forces, speed_weights, precision=highest, preferred_element_type=jnp.float32)
    speeds = velocity * (1.5 + jnp.tanh(drive_in))
    fastest = jnp.max(speeds)
    time_step = 0.8 / jnp.maximum(fastest, 1.0)
    fluxes = speeds[:, None] * macro_state
    state_after = jnp.roll(macro_state, -1, axis=0)
    flux_after = jnp.roll(fluxes, -1, axis=0)
    interface = 0.5 * (fluxes + flux_after) - 0.5 * fastest * (state_after - macro_state)
    interface_before = jnp.roll(interface, 1, axis=0)
    macro_next = macro_state - time_step * (interface - interface_before) + time_step * forces
    return macro_next, micro_final
```

```python
import functools

import jax
import jax.numpy as jnp
from jax import lax
from jax.experimental import pallas as pl
from jax.experimental.pallas import tpu as pltpu
from jax.sharding import Mesh
from jax.sharding import PartitionSpec as P

S = 12
STEPS = 4
MACRO = ("macro_0", "macro_1", "macro_2", "macro_3")
GROUP = ("macro_0", "macro_2", "macro_3")
IN_CHUNKS = (4, 4, 3, 1)
OUT_CHUNKS = (2, 5, 5)
HIGHEST = lax.Precision.HIGHEST
VM = pl.BlockSpec(memory_space=pltpu.VMEM)
ANY = pl.BlockSpec(memory_space=pl.ANY)


def call(body, outs, ins, specs=None, scratch=(), flops=0, aliases=None, out_specs=None, name=None):
    size = sum(a.size * a.dtype.itemsize for a in ins)
    return pl.pallas_call(
        body,
        out_shape=outs,
        in_specs=specs or [VM] * len(ins),
        out_specs=out_specs or jax.tree.map(lambda _: VM, outs),
        scratch_shapes=list(scratch),
        input_output_aliases=aliases or {},
        cost_estimate=pl.CostEstimate(flops=flops, bytes_accessed=size, transcendentals=0),
        name=name,
    )(*ins)


def f32dot(a, b, contract=((1,), (0,))):
    return lax.dot_general(a, b, (contract, ((), ())), precision=HIGHEST, preferred_element_type=jnp.float32)


def prepare(half, gathered, prop, fmap, macro, matrix_out, forcing_out):
    me = lax.axis_index("micro")
    pieces = gathered.shape[0]
    far_prop = gathered[:, :32, :].reshape(pieces * 32, half).astype(jnp.bfloat16)
    matrix_out[:, half:] = far_prop
    upper = matrix_out[:half, half:]
    lower = matrix_out[half:, half:]
    first = me == 0
    matrix_out[:half, half:] = jnp.where(first, upper, lower)
    matrix_out[half:, half:] = jnp.where(first, lower, upper)
    matrix_out[:half, :half] = jnp.where(first, prop[:half, :], prop[half:, :])
    matrix_out[half:, :half] = jnp.where(first, prop[half:, :], prop[:half, :])
    far_map = gathered[:, 32:40, :].reshape(pieces * 8, half)
    points = forcing_out.shape[0]
    mine = macro[pl.ds(pl.multiple_of(me * points, points), points), :]
    forcing_out[:, :half] = jnp.tanh(f32dot(mine, fmap[...]))
    forcing_out[:, half:] = jnp.tanh(f32dot(mine, far_map))


def advance(near, far, matrix, forcing, total_in, near_out, far_out, total_out, now, after):
    replicas, points, half = near.shape
    rows = replicas * points
    now[:, :half] = near[...].reshape(rows, half)
    now[:, half:] = far[...].reshape(rows, half)
    source, target = now, after
    for step in range(STEPS):
        for side in range(2):
            cols = slice(side * half, side * half + half)
            summed = jnp.dot(source[...], matrix[:, cols], preferred_element_type=jnp.float32)
            state = (summed.reshape(replicas, points, half) + forcing[:, cols][None]).astype(jnp.bfloat16)
            share = jnp.sum(jnp.tanh(state.astype(jnp.float32)), axis=0)
            before = total_in if step == 0 else total_out
            total_out[:, cols] = before[:, cols] + share
            if step == STEPS - 1:
                (near_out, far_out)[side][...] = state
            else:
                target[:, cols] = state.reshape(rows, half)
        source, target = target, source


def advance_last(
    near, far, matrix, forcing, total_in, gathered, readout, weights, velocity,
    near_out, far_out, message, total, now, after,
):
    advance(near, far, matrix, forcing, total_in, near_out, far_out, total, now, after)
    points, half = near.shape[1:]
    me = lax.axis_index("micro")
    averaged = total[...] / (STEPS * S)
    far_readout = gathered[:, 40:48, :].reshape(readout.shape)
    forces = f32dot(averaged[:, :half], readout[...], ((1,), (1,)))
    forces = forces + f32dot(averaged[:, half:], far_readout, ((1,), (1,)))
    message[:points, :] = forces
    drive = f32dot(forces, weights[...])
    base = velocity[pl.ds(pl.multiple_of(me * points, points), points), :]
    speeds = base * (1.5 + jnp.tanh(drive))
    row = lax.broadcasted_iota(jnp.int32, (8, speeds.shape[1]), 0)
    top = jnp.max(speeds, axis=0, keepdims=True)
    message[points:, :] = jnp.where(row == 0, top, jnp.where(row == 1, speeds[:1, :], speeds[points - 1 :, :]))


def combine(own, across, beside, both, out):
    me, low = lax.axis_index("micro"), lax.axis_index("macro_1")
    first, zero = me == 0, low == 0
    off = across.shape[0] - 8

    def rows(ref, base):
        return [ref[base + k : base + k + 1, :] for k in range(3)]

    a, b, c, d = rows(own, off), rows(across, off), rows(beside, 0), rows(both, 0)
    top = jnp.maximum(jnp.maximum(a[0], b[0]), jnp.maximum(c[0], d[0]))
    mine = (jnp.where(first, a[1], b[1]), jnp.where(first, b[2], a[2]))
    other = (jnp.where(first, c[1], d[1]), jnp.where(first, d[2], c[2]))
    block0 = [jnp.where(zero, x, y) for x, y in zip(mine, other)]
    block1 = [jnp.where(zero, y, x) for x, y in zip(mine, other)]
    lane = lax.broadcasted_iota(jnp.int32, top.shape, 1)
    value = top
    for k, v in enumerate(block0 + block1):
        value = jnp.where(lane == k + 1, v, value)
    out[...] = value


def finish(steps, table, own, across, macro, velocity, weights, behind, ahead, out, forces, state, flux):
    me = lax.axis_index("micro")
    points = own.shape[0] - 8
    count = out.shape[0]
    forces[pl.ds(pl.multiple_of(me * points, points), points), :] = own[:points, :]
    forces[pl.ds(pl.multiple_of((1 - me) * points, points), points), :] = across[:points, :]
    values = table[...]
    row = lax.broadcasted_iota(jnp.int32, values.shape, 0)
    lane = lax.broadcasted_iota(jnp.int32, values.shape, 1)

    def pick(mask):
        kept = jnp.where(mask, values, -jnp.inf)
        return jnp.max(jnp.max(kept, axis=0, keepdims=True), axis=1, keepdims=True)

    def coords(index):
        ys, xs, zs, cs = steps
        core = index % cs
        z = (index // cs) % zs
        low = (index // (cs * zs)) % xs
        y = index // (cs * zs * xs)
        return (y * zs + z) * cs + core, low

    ys, xs, zs, cs = steps
    total = ys * xs * zs * cs
    spot = [lax.axis_index(name) for name in MACRO]
    here = ((spot[0] * xs + spot[1]) * zs + spot[2]) * cs + spot[3]
    prev_row, prev_low = coords((here + total - 1) % total)
    next_row, next_low = coords((here + 1) % total)
    fastest = pick(lane == 0)
    prev_speed = pick((row == prev_row) & (lane == 2 + 2 * prev_low))
    next_speed = pick((row == next_row) & (lane == 1 + 2 * next_low))
    time_step = 0.8 / jnp.maximum(fastest, 1.0)
    speeds = velocity[...] * (1.5 + jnp.tanh(f32dot(forces[...], weights[...])))
    state[8 : 8 + count, :] = macro[...]
    flux[8 : 8 + count, :] = speeds * macro[...]
    state[7:8, :] = behind[...]
    flux[7:8, :] = prev_speed * behind[...]
    state[8 + count : 9 + count, :] = ahead[...]
    flux[8 + count : 9 + count, :] = next_speed * ahead[...]
    u0, u1, u2 = (state[k : k + count, :] for k in (7, 8, 9))
    f0, f1, f2 = (flux[k : k + count, :] for k in (7, 8, 9))
    high = 0.5 * (f1 + f2) - 0.5 * fastest * (u2 - u1)
    low = 0.5 * (f0 + f1) - 0.5 * fastest * (u1 - u0)
    out[...] = u1 - time_step * (high - low) + time_step * forces[...]


def place(plan, aliased, *refs):
    if aliased:
        refs = refs[1:]
    arrays, out, sems = refs[: len(plan)], refs[len(plan)], refs[len(plan) + 1]
    me = lax.axis_index("micro")
    copies = []
    for k, (array, (start, mine)) in enumerate(zip(arrays, plan)):
        replicas, points, _ = array.shape
        at = (me if mine else 1 - me) * points
        where = out.at[pl.ds(start, replicas), pl.ds(pl.multiple_of(at, points), points), :]
        copies.append(pltpu.make_async_copy(array, where, sems.at[k]))
    for copy in copies:
        copy.start()
    for copy in copies:
        copy.wait()


def placed_in(arrays, plan, out_type, out=None):
    ins = ([] if out is None else [out]) + list(arrays)
    return call(
        functools.partial(place, tuple(plan), out is not None),
        out_type,
        ins,
        specs=([] if out is None else [ANY]) + [VM] * len(arrays),
        out_specs=ANY,
        scratch=[pltpu.SemaphoreType.DMA((len(plan),))],
        aliases={} if out is None else {0: 0},
        name="place",
    )


def swapped(value):
    return lax.ppermute(value, "micro", [(0, 1), (1, 0)])


def shifted(value, steps):
    count = lax.axis_size(MACRO)
    return lax.ppermute(value, MACRO, [(k, (k + steps) % count) for k in range(count)])


def after(value, *others):
    return lax.optimization_barrier((value, *others))[0]


def starts(sizes):
    return [sum(sizes[:k]) for k in range(len(sizes))]


def shards(macro_state, micro_state, velocity, propagator, forcing_map, readout, speed_weights):
    f32, bf16 = jnp.float32, jnp.bfloat16
    me = lax.axis_index("micro")
    count, fields = macro_state.shape
    half = micro_state.shape[2]
    points = count // 2
    micro = jnp.transpose(micro_state, (1, 0, 2))

    def part(start, size, owner):
        return lax.dynamic_slice(micro, (start, owner * points, 0), (size, points, half))

    in_at = starts(IN_CHUNKS)
    arrived = [swapped(part(in_at[0], IN_CHUNKS[0], 1 - me))]
    zs, cs = lax.axis_size("macro_2"), lax.axis_size("macro_3")
    spot = lax.axis_index("macro_2") * cs + lax.axis_index("macro_3")
    pieces = zs * cs
    share = jnp.concatenate(
        [
            lax.dynamic_slice(a, (spot * (a.shape[0] // pieces), 0), (a.shape[0] // pieces, half)).astype(f32)
            for a in (propagator, forcing_map, readout)
        ]
    )
    far_share = swapped(share)
    for start, size in zip(in_at[1:], IN_CHUNKS[1:]):
        arrived.append(swapped(part(start, size, 1 - me)))
    gathered = lax.all_gather(far_share, ("macro_2", "macro_3"), axis=0, tiled=False)
    behind = shifted(macro_state[-1:], 1)
    ahead = shifted(macro_state[:1], -1)
    weights = jnp.broadcast_to(speed_weights[:, None], (fields, 128))
    speed_base = jnp.broadcast_to(velocity[:, None], (count, 128))

    matrix, forcing = call(
        functools.partial(prepare, half),
        (jax.ShapeDtypeStruct((2 * half, 2 * half), bf16), jax.ShapeDtypeStruct((points, 2 * half), f32)),
        [gathered, propagator, forcing_map, macro_state],
        flops=10**8,
        name="prepare",
    )
    total = jnp.zeros((points, 2 * half), f32)
    near_parts, far_parts = [], []
    last = len(IN_CHUNKS) - 1
    message = None
    for k, (start, size) in enumerate(zip(in_at, IN_CHUNKS)):
        chunk = jax.ShapeDtypeStruct((size, points, half), bf16)
        sums = jax.ShapeDtypeStruct(total.shape, f32)
        ins = [part(start, size, me), arrived[k], matrix, forcing, total]
        buffers = [pltpu.VMEM((size * points, 2 * half), bf16)] * 2
        work = 2 * STEPS * size * points * (2 * half) ** 2
        if k < last:
            near, far, total = call(
                advance, (chunk, chunk, sums), ins, scratch=buffers, flops=work, aliases={4: 2}, name=f"advance_{k}"
            )
        else:
            near, far, message = call(
                advance_last,
                (chunk, chunk, jax.ShapeDtypeStruct((points + 8, 128), f32)),
                [*ins, gathered, readout, weights, speed_base],
                scratch=[pltpu.VMEM(total.shape, f32), *buffers],
                flops=work,
                name="advance_last",
            )
        near_parts.append(near)
        far_parts.append(far)

    everything = jnp.concatenate(far_parts[:-1], axis=0)
    own_note = message[points:]
    across = swapped(message)
    beside = lax.ppermute(own_note, "macro_1", [(0, 1), (1, 0)])
    both = lax.ppermute(own_note, ("macro_1", "micro"), [(k, 3 - k) for k in range(4)])
    row = call(
        combine, jax.ShapeDtypeStruct((1, 128), f32), [message, across, beside, both], name="combine"
    )
    group = lax.axis_size(GROUP)
    table = lax.all_to_all(jnp.broadcast_to(row[None], (group, 1, 128)), GROUP, split_axis=0, concat_axis=0, tiled=True)
    table = table.reshape(group, 128)

    returned = [swapped(f) for f in far_parts]
    sizes = tuple(lax.axis_size(name) for name in MACRO)
    macro_next = call(
        functools.partial(finish, sizes),
        jax.ShapeDtypeStruct((count, fields), f32),
        [table, message, across, macro_state, speed_base, weights, behind, ahead],
        scratch=[pltpu.VMEM((count, 128), f32), pltpu.VMEM((count + 16, 128), f32), pltpu.VMEM((count + 16, 128), f32)],
        name="finish",
    )
    out_type = jax.ShapeDtypeStruct(micro.shape, bf16)
    out = placed_in(near_parts, [(s, True) for s in in_at], out_type)
    for start, value in zip(in_at, returned):
        out = placed_in([value], [(start, False)], out_type, out)
    return macro_next, jnp.transpose(out, (1, 0, 2))


def solution(mesh):
    torus = Mesh(
        mesh.devices.reshape(4, 2, 8, 2, mesh.shape["micro"]),
        ("macro_0", "macro_1", "macro_2", "macro_3", "micro"),
    )
    placed = (
        P(MACRO, None),
        P(MACRO, None, "micro"),
        P(MACRO),
        P(None, "micro"),
        P(None, "micro"),
        P(None, "micro"),
        P(),
    )
    return jax.shard_map(
        shards,
        mesh=torus,
        in_specs=placed,
        out_specs=(P(MACRO, None), P(MACRO, None, "micro")),
        check_vma=False,
    )
```

```python
import functools

import jax
import jax.numpy as jnp
from jax import lax
from jax.experimental import pallas as pl
from jax.experimental.pallas import tpu as pltpu
from jax.sharding import Mesh
from jax.sharding import PartitionSpec as P


S = 12
STEPS = 4
MACRO = ("macro_0", "macro_1", "macro_2", "macro_3")
GROUP = ("macro_0", "macro_2", "macro_3")
CHUNKS = (2, 4, 3, 2, 1)
GROUPS = ((0,), (1, 2), (3, 4))
HIGHEST = lax.Precision.HIGHEST
VM = pl.BlockSpec(memory_space=pltpu.VMEM)
ANY = pl.BlockSpec(memory_space=pl.ANY)
HBM = pl.BlockSpec(memory_space=pltpu.HBM)
VMEM_BYTES = 6 * 2**20
FIRST_BYTES = 64_500_000
REST_BYTES = 60_500_000


def call(body, outs, ins, specs=None, scratch=(), flops=0, aliases=None, out_specs=None, limit=None):
    size = sum(a.size * a.dtype.itemsize for a in ins)
    return pl.pallas_call(
        body,
        out_shape=outs,
        in_specs=specs or [VM] * len(ins),
        out_specs=out_specs or jax.tree.map(lambda _: VM, outs),
        scratch_shapes=list(scratch),
        input_output_aliases=aliases or {},
        compiler_params=pltpu.CompilerParams(vmem_limit_bytes=limit or VMEM_BYTES),
        cost_estimate=pl.CostEstimate(flops=flops, bytes_accessed=size, transcendentals=0),
    )(*ins)


def f32dot(a, b, contract=((1,), (0,))):
    return lax.dot_general(a, b, (contract, ((), ())), precision=HIGHEST, preferred_element_type=jnp.float32)


def eighth():
    return (lax.axis_index("macro_2") % 4) * 2 + lax.axis_index("macro_3")


def slice_copies(plan, micro, outs, sems):
    me = lax.axis_index("micro")
    copies = []
    for k, ((start, mine), out) in enumerate(zip(plan, outs)):
        replicas, points, _ = out.shape
        at = (me if mine else 1 - me) * points
        where = micro.at[pl.ds(start, replicas), pl.ds(pl.multiple_of(at, points), points), :]
        copies.append(pltpu.make_async_copy(where, out, sems.at[k]))
    return copies


def cut_first(plan, micro, prop, fmap, readout, out, share, maps, sems, more):
    e = eighth()
    small = pl.ds(pl.multiple_of(e * 16, 16), 16)
    copies = slice_copies(plan, micro, [out], sems)
    copies += [
        pltpu.make_async_copy(fmap.at[small, :], maps.at[0], more.at[0]),
        pltpu.make_async_copy(readout.at[small, :], maps.at[1], more.at[1]),
        pltpu.make_async_copy(
            prop.at[pl.ds(pl.multiple_of(e * 64, 64), 64), :], share.at[pl.ds(0, 64), :], more.at[2]
        ),
    ]
    for copy in copies:
        copy.start()
    for copy in copies:
        copy.wait()
    for k in range(2):
        rows = maps[k]
        high = rows.astype(jnp.bfloat16)
        share[64 + 32 * k : 80 + 32 * k, :] = high
        share[80 + 32 * k : 96 + 32 * k, :] = (rows - high.astype(jnp.float32)).astype(jnp.bfloat16)


def cut_rest(plan, micro, _, *refs):
    copies = slice_copies(plan, micro, refs[:-1], refs[-1])
    for copy in copies:
        copy.start()
    for copy in copies:
        copy.wait()


def prepare(half, s0, s1, s2, s3, prop, fmap, macro, matrix_out, forcing_out, readout_out, far_map):
    me, e = lax.axis_index("micro"), eighth()
    points = forcing_out.shape[0]
    core, low_z, mid_z = e % 2, (e // 2) % 2, e // 4
    for k, pair in enumerate((s0, s1, s2, s3)):
        c = core if k % 2 == 0 else 1 - core
        z = low_z if k < 2 else 1 - low_z
        for t in range(2):
            share = pair.at[t]
            y = mid_z if t == 0 else 1 - mid_z
            y_row = (y + me) % 2
            spot = pl.ds(pl.multiple_of((y_row * 4 + z * 2 + c) * 64, 64), 64)
            matrix_out[spot, half:] = share[:64, :]
            at = pl.ds(pl.multiple_of((y * 4 + z * 2 + c) * 16, 16), 16)
            far_map[at, :] = share[64:80, :].astype(jnp.float32) + share[80:96, :].astype(jnp.float32)
            readout_out[at, :] = share[96:112, :].astype(jnp.float32) + share[112:128, :].astype(jnp.float32)
    matrix_out[:half, :half] = prop[pl.ds(pl.multiple_of(me * half, half), half), :]
    matrix_out[half:, :half] = prop[pl.ds(pl.multiple_of((1 - me) * half, half), half), :]
    mine = macro[pl.ds(pl.multiple_of(me * points, points), points), :]
    forcing_out[:, :half] = jnp.tanh(f32dot(mine, fmap[...]))
    forcing_out[:, half:] = jnp.tanh(f32dot(mine, far_map[...]))


def steps_of(start, at, micro, far, matrix, forcing, total_in, out, far_out, total_out, now, after, keep, sem):
    replicas, points, half = far.shape
    rows = replicas * points
    spot = pl.ds(pl.multiple_of(lax.axis_index("micro") * points, points), points)
    near = pltpu.make_async_copy(micro.at[pl.ds(start, replicas), spot, :], keep, sem.at[1])
    near.start()
    now[:, half:] = far[...].reshape(rows, half)
    near.wait()
    now[:, :half] = keep[...].reshape(rows, half)
    source, target = now, after
    copy = pltpu.make_async_copy(keep, out.at[pl.ds(start, replicas), spot, :], sem.at[0])
    for step in range(STEPS):
        for side in range(2):
            cols = slice(side * half, side * half + half)
            summed = jnp.dot(source[...], matrix[:, cols], preferred_element_type=jnp.float32)
            state = (summed.reshape(replicas, points, half) + forcing[:, cols][None]).astype(jnp.bfloat16)
            share = jnp.sum(jnp.tanh(state.astype(jnp.float32)), axis=0)
            if step > 0:
                share = total_out[:, cols] + share
            elif total_in is not None:
                share = total_in[:, cols] + share
            total_out[:, cols] = share
            if step < STEPS - 1:
                target[:, cols] = state.reshape(rows, half)
            elif side == 0:
                keep[...] = state
                copy.start()
            else:
                far_out[at : at + replicas] = state
        source, target = target, source
    return copy


def advance(start, at, inner, has_group, micro, far, matrix, forcing, *refs):
    total_in = refs[1] if inner else None
    out, far_out, total, now, after, keep, sem = refs[2 * inner + has_group :]
    copy = steps_of(start, at, micro, far, matrix, forcing, total_in, out, far_out, total, now, after, keep, sem)
    copy.wait()


def advance_last(start, at, has_group, micro, far, matrix, forcing, _, total_in, *refs):
    readout, far_readout, weights, velocity, macro, out, far_out, message, note = refs[has_group : has_group + 9]
    total, now, after, keep, sem = refs[has_group + 9 :]
    copy = steps_of(start, at, micro, far, matrix, forcing, total_in, out, far_out, total, now, after, keep, sem)
    points, half = far.shape[1:]
    me = lax.axis_index("micro")
    averaged = total[...] / (STEPS * S)
    forces = f32dot(averaged[:, :half], readout[...], ((1,), (1,)))
    forces = forces + f32dot(averaged[:, half:], far_readout[...], ((1,), (1,)))
    forces = forces.astype(jnp.bfloat16)
    message[:points, :] = forces
    drive = f32dot(forces.astype(jnp.float32), weights[...])
    base = velocity[pl.ds(pl.multiple_of(me * points, points), points), :]
    speeds = base * (1.5 + jnp.tanh(drive))
    row = lax.broadcasted_iota(jnp.int32, (8, speeds.shape[1]), 0)
    top = jnp.max(speeds, axis=0, keepdims=True)
    values = jnp.where(row == 0, top, jnp.where(row == 1, speeds[:1, :], speeds[points - 1 :, :]))
    count = macro.shape[0]
    note[...] = jnp.where(row == 3, macro[:1, :], jnp.where(row == 4, macro[count - 1 :, :], values))
    for k in range(3):
        piece = values.astype(jnp.bfloat16)
        message[points + 16 * k : points + 8 + 16 * k, :] = piece
        values = values - piece.astype(jnp.float32)
    copy.wait()


def group_spot(sizes, index):
    _, xs, zs, cs = sizes
    y = index // (cs * zs * xs)
    return (y * zs + (index // cs) % zs) * cs + index % cs, (index // (cs * zs)) % xs


def combine(sizes, own, across, beside, both, out):
    ys, xs, zs, cs = sizes
    me = lax.axis_index("micro")
    y, low, z, core = (lax.axis_index(name) for name in MACRO)
    first, zero = me == 0, low == 0
    off = across.shape[0] - 48
    parts = [across[off + 16 * k : off + 8 + 16 * k, :].astype(jnp.float32) for k in range(3)]
    far = parts[0] + parts[1] + parts[2]
    a, c, d = ([ref[k : k + 1, :] for k in range(3)] for ref in (own, beside, both))
    b = [far[k : k + 1, :] for k in range(3)]
    top = jnp.maximum(jnp.maximum(a[0], b[0]), jnp.maximum(c[0], d[0]))
    mine = (jnp.where(first, a[1], b[1]), jnp.where(first, b[2], a[2]))
    other = (jnp.where(first, c[1], d[1]), jnp.where(first, d[2], c[2]))
    block0 = [jnp.where(zero, x, v) for x, v in zip(mine, other)]
    block1 = [jnp.where(zero, v, x) for x, v in zip(mine, other)]
    lane = lax.broadcasted_iota(jnp.int32, top.shape, 1)
    value = top
    for k, v in enumerate(block0 + block1):
        value = jnp.where(lane == k + 1, v, value)
    total = ys * xs * zs * cs
    up = (z == zs - 1) & (core == cs - 1)
    down = (z == 0) & (core == 0)
    after_low = jnp.where(up, 1 - low, low)
    before_low = jnp.where(down, 1 - low, low)
    after_spot, _ = group_spot(sizes, (((y * xs + after_low) * zs + z) * cs + core + 1) % total)
    before_spot, _ = group_spot(sizes, (((y * xs + before_low) * zs + z) * cs + core + total - 1) % total)
    last_state = jnp.where(up, beside[4:5, :], own[4:5, :])
    first_state = jnp.where(down, beside[3:4, :], own[3:4, :])
    row = lax.broadcasted_iota(jnp.int32, out.shape, 0)
    rows = jnp.where(row % 2 == 0, value, 0.0)
    rows = jnp.where(row == 2 * after_spot + 1, last_state, rows)
    out[...] = jnp.where(row == 2 * before_spot + 1, first_state, rows)


def finish(sizes, table, own, across, macro, velocity, weights, out, forces, state, flux):
    me = lax.axis_index("micro")
    points = own.shape[0] - 48
    count = out.shape[0]
    forces[pl.ds(pl.multiple_of(me * points, points), points), :] = own[:points, :].astype(jnp.float32)
    forces[pl.ds(pl.multiple_of((1 - me) * points, points), points), :] = across[:points, :].astype(jnp.float32)
    values = table[...]
    row = lax.broadcasted_iota(jnp.int32, values.shape, 0)
    lane = lax.broadcasted_iota(jnp.int32, values.shape, 1)

    def pick(mask):
        kept = jnp.where(mask, values, -jnp.inf)
        return jnp.max(jnp.max(kept, axis=0, keepdims=True), axis=1, keepdims=True)

    ys, xs, zs, cs = sizes
    total = ys * xs * zs * cs
    spot = [lax.axis_index(name) for name in MACRO]
    here = ((spot[0] * xs + spot[1]) * zs + spot[2]) * cs + spot[3]
    prev_row, prev_low = group_spot(sizes, (here + total - 1) % total)
    next_row, next_low = group_spot(sizes, (here + 1) % total)
    fastest = pick((lane == 0) & (row % 2 == 0))
    prev_speed = pick((row == 2 * prev_row) & (lane == 2 + 2 * prev_low))
    next_speed = pick((row == 2 * next_row) & (lane == 1 + 2 * next_low))
    behind = table[pl.ds(2 * prev_row + 1, 1), :]
    ahead = table[pl.ds(2 * next_row + 1, 1), :]
    time_step = 0.8 / jnp.maximum(fastest, 1.0)
    speeds = velocity[...] * (1.5 + jnp.tanh(f32dot(forces[...], weights[...])))
    state[8 : 8 + count, :] = macro[...]
    flux[8 : 8 + count, :] = speeds * macro[...]
    state[7:8, :] = behind
    flux[7:8, :] = prev_speed * behind
    state[8 + count : 9 + count, :] = ahead
    flux[8 + count : 9 + count, :] = next_speed * ahead
    u0, u1, u2 = (state[k : k + count, :] for k in (7, 8, 9))
    f0, f1, f2 = (flux[k : k + count, :] for k in (7, 8, 9))
    high = 0.5 * (f1 + f2) - 0.5 * fastest * (u2 - u1)
    low = 0.5 * (f0 + f1) - 0.5 * fastest * (u1 - u0)
    out[...] = u1 - time_step * (high - low) + time_step * forces[...]


def place(start, array, _, out, sem):
    replicas, points, _ = array.shape
    spot = pl.ds(pl.multiple_of((1 - lax.axis_index("micro")) * points, points), points)
    copy = pltpu.make_async_copy(array, out.at[pl.ds(start, replicas), spot, :], sem.at[0])
    copy.start()
    copy.wait()


def placed_in(array, start, out):
    return call(
        functools.partial(place, start),
        jax.ShapeDtypeStruct(out.shape, out.dtype),
        [array, out],
        specs=[VM, HBM],
        out_specs=HBM,
        scratch=[pltpu.SemaphoreType.DMA((1,))],
        aliases={1: 0},
    )


def swapped(value):
    return lax.ppermute(value, "micro", [(0, 1), (1, 0)])


def near_copy(value, low_z, core):
    count = lax.axis_size("macro_2")
    spots = [(z, c) for z in range(count) for c in range(2)]
    pairs = [(z * 2 + c, (z ^ low_z) * 2 + (c ^ core)) for z, c in spots]
    return lax.ppermute(value, ("macro_2", "macro_3"), pairs)


def starts(sizes):
    return [sum(sizes[:k]) for k in range(len(sizes))]


def shards(macro_state, micro_state, velocity, propagator, forcing_map, readout, speed_weights):
    f32, bf16 = jnp.float32, jnp.bfloat16
    count, fields = macro_state.shape
    half = micro_state.shape[2]
    points = count // 2
    micro = jnp.transpose(micro_state, (1, 0, 2))

    begin = starts(CHUNKS)
    chunks = [jax.ShapeDtypeStruct((size, points, half), bf16) for size in CHUNKS]
    first, share = call(
        functools.partial(cut_first, ((0, False),)),
        (chunks[0], jax.ShapeDtypeStruct((128, half), bf16)),
        [micro, propagator, forcing_map, readout],
        specs=[HBM] * 4,
        scratch=[pltpu.VMEM((2, 16, half), f32), pltpu.SemaphoreType.DMA((1,)), pltpu.SemaphoreType.DMA((3,))],
        limit=FIRST_BYTES,
    )
    plan = tuple((at, False) for at in begin[1:])
    rest = call(
        functools.partial(cut_rest, plan),
        tuple(chunks[1:]),
        [micro, share],
        specs=[HBM, ANY],
        scratch=[pltpu.SemaphoreType.DMA((len(plan),))],
        limit=REST_BYTES,
    )
    arrived = []
    for value in [first, *rest]:
        arrived.append(swapped(value))
    share = swapped(share)
    other = near_copy(share, 2, 0)
    share = jnp.stack([share, other])
    shares = [share]
    for z, c in ((0, 1), (1, 0), (1, 1)):
        shares.append(near_copy(share, z, c))
    weights = jnp.broadcast_to(speed_weights[:, None], (fields, 128))
    speed_base = jnp.broadcast_to(velocity[:, None], (count, 128))
    sums = jax.ShapeDtypeStruct((points, 2 * half), f32)
    matrix, forcing, far_readout = call(
        functools.partial(prepare, half),
        (jax.ShapeDtypeStruct((2 * half, 2 * half), bf16), sums, jax.ShapeDtypeStruct(readout.shape, f32)),
        [*shares, propagator, forcing_map, macro_state],
        scratch=[pltpu.VMEM(forcing_map.shape, f32)],
        flops=10**8,
    )
    out_type = jax.ShapeDtypeStruct(micro.shape, bf16)
    far_parts = []
    out = total = None
    for members in GROUPS:
        size_of_group = sum(CHUNKS[k] for k in members)
        group, at = None, 0
        for k in members:
            size = CHUNKS[k]
            whole = jax.ShapeDtypeStruct((size_of_group, points, half), bf16)
            ins, specs, aliases = [micro, arrived[k], matrix, forcing], [HBM] + [VM] * 3, {}
            inner = out is not None
            if inner:
                aliases = {4: 0, 5: 2}
                ins += [out, total]
                specs += [HBM, VM]
            if group is not None:
                aliases[len(ins)] = 1
                ins.append(group)
                specs.append(VM)
            scratch = [pltpu.VMEM((size * points, 2 * half), bf16)] * 2
            scratch += [pltpu.VMEM((size, points, half), bf16), pltpu.SemaphoreType.DMA((2,))]
            work = 2 * STEPS * size * points * (2 * half) ** 2
            if k < len(CHUNKS) - 1:
                out, group, total = call(
                    functools.partial(advance, begin[k], at, inner, group is not None),
                    (out_type, whole, sums),
                    ins,
                    specs=specs,
                    out_specs=(HBM, VM, VM),
                    scratch=scratch,
                    flops=work,
                    aliases=aliases,
                )
            else:
                aliases.pop(5)
                out, group, message, note = call(
                    functools.partial(advance_last, begin[k], at, group is not None),
                    (
                        out_type,
                        whole,
                        jax.ShapeDtypeStruct((points + 48, 128), bf16),
                        jax.ShapeDtypeStruct((8, 128), f32),
                    ),
                    [*ins, readout, far_readout, weights, speed_base, macro_state],
                    specs=specs + [VM] * 5,
                    out_specs=(HBM, VM, VM, VM),
                    scratch=[pltpu.VMEM(sums.shape, f32), *scratch],
                    flops=work,
                    aliases=aliases,
                )
            at += size
        far_parts.append(group)

    across = swapped(message)
    beside = lax.ppermute(note, "macro_1", [(0, 1), (1, 0)])
    both = lax.ppermute(note, ("macro_1", "micro"), [(k, 3 - k) for k in range(4)])
    returned = []
    for value in far_parts:
        returned.append(swapped(value))
    group = lax.axis_size(GROUP)
    sizes = tuple(lax.axis_size(name) for name in MACRO)
    rows = call(
        functools.partial(combine, sizes), jax.ShapeDtypeStruct((2 * group, 128), f32), [note, across, beside, both]
    )
    table = lax.all_to_all(rows.reshape(group, 2, 128), GROUP, split_axis=0, concat_axis=0, tiled=True)
    table = table.reshape(2 * group, 128)
    macro_next = call(
        functools.partial(finish, sizes),
        jax.ShapeDtypeStruct((count, fields), f32),
        [table, message, across, macro_state, speed_base, weights],
        scratch=[pltpu.VMEM((count, 128), f32), pltpu.VMEM((count + 16, 128), f32), pltpu.VMEM((count + 16, 128), f32)],
    )
    for members, value in zip(GROUPS, returned):
        out = placed_in(value, begin[members[0]], out)
    return macro_next, jnp.transpose(out, (1, 0, 2))


def solution(mesh):
    torus = Mesh(
        mesh.devices.reshape(4, 2, 8, 2, mesh.shape["micro"]),
        ("macro_0", "macro_1", "macro_2", "macro_3", "micro"),
    )
    placed = (
        P(MACRO, None),
        P(MACRO, None, "micro"),
        P(MACRO),
        P(None, "micro"),
        P(None, "micro"),
        P(None, "micro"),
        P(),
    )
    return jax.shard_map(
        shards,
        mesh=torus,
        in_specs=placed,
        out_specs=(P(MACRO, None), P(MACRO, None, "micro")),
        check_vma=False,
    )
```

```python
import functools

import jax
import jax.numpy as jnp
from jax import lax
from jax.experimental import pallas as pl
from jax.experimental.pallas import tpu as pltpu
from jax.sharding import Mesh
from jax.sharding import PartitionSpec as P


S = 12
STEPS = 4
MACRO = ("macro_0", "macro_1", "macro_2", "macro_3")
GROUP = ("macro_0", "macro_2", "macro_3")
CHUNKS = (1, 2, 5, 3, 1)
UNITS = ((0, 1), (2,), (3,), (4,))
GROUPS = ((0,), (1, 2, 3))
SHARE = 128
HIGHEST = lax.Precision.HIGHEST
VM = pl.BlockSpec(memory_space=pltpu.VMEM)
ANY = pl.BlockSpec(memory_space=pl.ANY)
HBM = pl.BlockSpec(memory_space=pltpu.HBM)
VMEM_BYTES = 6 * 2**20
FIRST_BYTES = 64_500_000
REST_BYTES = 60_500_000


def call(body, outs, ins, specs=None, scratch=(), flops=0, aliases=None, out_specs=None, limit=None):
    size = sum(a.size * a.dtype.itemsize for a in ins)
    return pl.pallas_call(
        body,
        out_shape=outs,
        in_specs=specs or [VM] * len(ins),
        out_specs=out_specs or jax.tree.map(lambda _: VM, outs),
        scratch_shapes=list(scratch),
        input_output_aliases=aliases or {},
        compiler_params=pltpu.CompilerParams(vmem_limit_bytes=limit or VMEM_BYTES),
        cost_estimate=pl.CostEstimate(flops=flops, bytes_accessed=size, transcendentals=0),
    )(*ins)


def f32dot(a, b, contract=((1,), (0,))):
    return lax.dot_general(a, b, (contract, ((), ())), precision=HIGHEST, preferred_element_type=jnp.float32)


def eighth():
    return (lax.axis_index("macro_2") % 4) * 2 + lax.axis_index("macro_3")


def slice_copies(plan, micro, outs, sems):
    me = lax.axis_index("micro")
    copies = []
    for k, ((start, mine), out) in enumerate(zip(plan, outs)):
        replicas, points, _ = out.shape
        at = (me if mine else 1 - me) * points
        where = micro.at[pl.ds(start, replicas), pl.ds(pl.multiple_of(at, points), points), :]
        copies.append(pltpu.make_async_copy(where, out, sems.at[k]))
    return copies


def cut_first(replicas, points, micro, prop, fmap, readout, out, maps, sems, more):
    e = eighth()
    base = replicas * points
    small = pl.ds(pl.multiple_of(e * 16, 16), 16)
    spot = pl.ds(pl.multiple_of((1 - lax.axis_index("micro")) * points, points), points)
    copies = [
        pltpu.make_async_copy(micro.at[k, spot, :], out.at[pl.ds(k * points, points), :], sems.at[k])
        for k in range(replicas)
    ]
    copies += [
        pltpu.make_async_copy(fmap.at[small, :], maps.at[0], more.at[0]),
        pltpu.make_async_copy(readout.at[small, :], maps.at[1], more.at[1]),
        pltpu.make_async_copy(
            prop.at[pl.ds(pl.multiple_of(e * 64, 64), 64), :], out.at[pl.ds(base, 64), :], more.at[2]
        ),
    ]
    for copy in copies:
        copy.start()
    for copy in copies:
        copy.wait()
    for k in range(2):
        rows = maps[k]
        high = rows.astype(jnp.bfloat16)
        at = base + 64 + 32 * k
        out[at : at + 16, :] = high
        out[at + 16 : at + 32, :] = (rows - high.astype(jnp.float32)).astype(jnp.bfloat16)


def cut_rest(plan, micro, _, *refs):
    copies = slice_copies(plan, micro, refs[:-1], refs[-1])
    for copy in copies:
        copy.start()
    for copy in copies:
        copy.wait()


def prepare(half, s0, s1, s2, s3, prop, fmap, macro, matrix_out, forcing_out, readout_out, far_map):
    me, e = lax.axis_index("micro"), eighth()
    points = forcing_out.shape[0]
    core, low_z, mid_z = e % 2, (e // 2) % 2, e // 4
    for k, pair in enumerate((s0, s1, s2, s3)):
        c = core if k % 2 == 0 else 1 - core
        z = low_z if k < 2 else 1 - low_z
        for t in range(2):
            share = pair.at[t]
            y = mid_z if t == 0 else 1 - mid_z
            y_row = (y + me) % 2
            spot = pl.ds(pl.multiple_of((y_row * 4 + z * 2 + c) * 64, 64), 64)
            matrix_out[spot, half:] = share[:64, :]
            at = pl.ds(pl.multiple_of((y * 4 + z * 2 + c) * 16, 16), 16)
            far_map[at, :] = share[64:80, :].astype(jnp.float32) + share[80:96, :].astype(jnp.float32)
            readout_out[at, :] = share[96:112, :].astype(jnp.float32) + share[112:128, :].astype(jnp.float32)
    matrix_out[:half, :half] = prop[pl.ds(pl.multiple_of(me * half, half), half), :]
    matrix_out[half:, :half] = prop[pl.ds(pl.multiple_of((1 - me) * half, half), half), :]
    mine = macro[pl.ds(pl.multiple_of(me * points, points), points), :]
    forcing_out[:, :half] = jnp.tanh(f32dot(mine, fmap[...]))
    forcing_out[:, half:] = jnp.tanh(f32dot(mine, far_map[...]))


def steps_of(start, at, micro, fars, matrix, forcing, total_in, out, far_out, total_out, now, after, keep, sem):
    points, half = far_out.shape[1:]
    replicas = keep.shape[0]
    rows = replicas * points
    spot = pl.ds(pl.multiple_of(lax.axis_index("micro") * points, points), points)
    near = pltpu.make_async_copy(micro.at[pl.ds(start, replicas), spot, :], keep, sem.at[1])
    near.start()
    row = 0
    for far in fars:
        count = far.shape[0] * points if len(far.shape) == 3 else far.shape[0] - SHARE
        now[row : row + count, half:] = far[:count, :] if len(far.shape) == 2 else far[...].reshape(count, half)
        row += count
    near.wait()
    now[:, :half] = keep[...].reshape(rows, half)
    source, target = now, after
    copy = pltpu.make_async_copy(keep, out.at[pl.ds(start, replicas), spot, :], sem.at[0])
    for step in range(STEPS):
        for side in range(2):
            cols = slice(side * half, side * half + half)
            summed = jnp.dot(source[...], matrix[:, cols], preferred_element_type=jnp.float32)
            state = (summed.reshape(replicas, points, half) + forcing[:, cols][None]).astype(jnp.bfloat16)
            share = jnp.sum(jnp.tanh(state.astype(jnp.float32)), axis=0)
            if step > 0:
                share = total_out[:, cols] + share
            elif total_in is not None:
                share = total_in[:, cols] + share
            total_out[:, cols] = share
            if step < STEPS - 1:
                target[:, cols] = state.reshape(rows, half)
            elif side == 0:
                keep[...] = state
                copy.start()
            else:
                far_out[at : at + replicas] = state
        source, target = target, source
    return copy


def advance(start, at, parts, inner, has_group, micro, *refs):
    fars, (matrix, forcing), refs = refs[:parts], refs[parts : parts + 2], refs[parts + 2 :]
    total_in = refs[1] if inner else None
    out, far_out, total, now, after, keep, sem = refs[2 * inner + has_group :]
    copy = steps_of(start, at, micro, fars, matrix, forcing, total_in, out, far_out, total, now, after, keep, sem)
    copy.wait()


def spread(row):
    return jnp.broadcast_to(row, (row.shape[1], row.shape[1])).T


def base_speeds(velocity, start, count):
    return jnp.concatenate([spread(velocity[pl.ds(start + k, 1), :]) for k in range(count)], axis=0)


def advance_last(start, at, parts, has_group, micro, *refs):
    fars, (matrix, forcing), refs = refs[:parts], refs[parts : parts + 2], refs[parts + 3 :]
    total_in, refs = refs[0], refs[1 + has_group :]
    readout, far_readout, weights, velocity, macro, out, far_out, message, note = refs[:9]
    total, now, after, keep, sem = refs[9:]
    copy = steps_of(start, at, micro, fars, matrix, forcing, total_in, out, far_out, total, now, after, keep, sem)
    points, half = far_out.shape[1:]
    me = lax.axis_index("micro")
    averaged = total[...] / (STEPS * S)
    forces = f32dot(averaged[:, :half], readout[...], ((1,), (1,)))
    forces = forces + f32dot(averaged[:, half:], far_readout[...], ((1,), (1,)))
    forces = forces.astype(jnp.bfloat16)
    message[:points, :] = forces
    drive = f32dot(forces.astype(jnp.float32), spread(weights[...]))
    blocks = points // 128
    speeds = base_speeds(velocity, me * blocks, blocks) * (1.5 + jnp.tanh(drive))
    row = lax.broadcasted_iota(jnp.int32, (8, speeds.shape[1]), 0)
    top = jnp.max(speeds, axis=0, keepdims=True)
    values = jnp.where(row == 0, top, jnp.where(row == 1, speeds[:1, :], speeds[points - 1 :, :]))
    count = macro.shape[0]
    note[...] = jnp.where(row == 3, macro[:1, :], jnp.where(row == 4, macro[count - 1 :, :], values))
    for k in range(3):
        piece = values.astype(jnp.bfloat16)
        message[points + 16 * k : points + 8 + 16 * k, :] = piece
        values = values - piece.astype(jnp.float32)
    copy.wait()


def group_spot(sizes, index):
    _, xs, zs, cs = sizes
    y = index // (cs * zs * xs)
    return (y * zs + (index // cs) % zs) * cs + index % cs, (index // (cs * zs)) % xs


def combine(sizes, own, across, beside, both, out):
    ys, xs, zs, cs = sizes
    me = lax.axis_index("micro")
    y, low, z, core = (lax.axis_index(name) for name in MACRO)
    first, zero = me == 0, low == 0
    off = across.shape[0] - 48
    parts = [across[off + 16 * k : off + 8 + 16 * k, :].astype(jnp.float32) for k in range(3)]
    far = parts[0] + parts[1] + parts[2]
    a, c, d = ([ref[k : k + 1, :] for k in range(3)] for ref in (own, beside, both))
    b = [far[k : k + 1, :] for k in range(3)]
    top = jnp.maximum(jnp.maximum(a[0], b[0]), jnp.maximum(c[0], d[0]))
    mine = (jnp.where(first, a[1], b[1]), jnp.where(first, b[2], a[2]))
    other = (jnp.where(first, c[1], d[1]), jnp.where(first, d[2], c[2]))
    block0 = [jnp.where(zero, x, v) for x, v in zip(mine, other)]
    block1 = [jnp.where(zero, v, x) for x, v in zip(mine, other)]
    lane = lax.broadcasted_iota(jnp.int32, top.shape, 1)
    value = top
    for k, v in enumerate(block0 + block1):
        value = jnp.where(lane == k + 1, v, value)
    total = ys * xs * zs * cs
    up = (z == zs - 1) & (core == cs - 1)
    down = (z == 0) & (core == 0)
    after_low = jnp.where(up, 1 - low, low)
    before_low = jnp.where(down, 1 - low, low)
    after_spot, _ = group_spot(sizes, (((y * xs + after_low) * zs + z) * cs + core + 1) % total)
    before_spot, _ = group_spot(sizes, (((y * xs + before_low) * zs + z) * cs + core + total - 1) % total)
    last_state = jnp.where(up, beside[4:5, :], own[4:5, :])
    first_state = jnp.where(down, beside[3:4, :], own[3:4, :])
    row = lax.broadcasted_iota(jnp.int32, out.shape, 0)
    rows = jnp.where(row % 2 == 0, value, 0.0)
    rows = jnp.where(row == 2 * after_spot + 1, last_state, rows)
    out[...] = jnp.where(row == 2 * before_spot + 1, first_state, rows)


def before_finish(own, across, macro, velocity, weights, packed, forces, flux):
    me = lax.axis_index("micro")
    points = own.shape[0] - 48
    count = macro.shape[0]
    forces[pl.ds(pl.multiple_of(me * points, points), points), :] = own[:points, :].astype(jnp.float32)
    forces[pl.ds(pl.multiple_of((1 - me) * points, points), points), :] = across[:points, :].astype(jnp.float32)
    flux[:8, :] = jnp.zeros((8, flux.shape[1]), jnp.float32)
    flux[8 + count :, :] = jnp.zeros((8, flux.shape[1]), jnp.float32)
    base = base_speeds(velocity, 0, count // 128)
    flux[8 : 8 + count, :] = base * (1.5 + jnp.tanh(f32dot(forces[...], spread(weights[...])))) * macro[...]
    packed[:count, :] = macro[...]
    packed[count:, :] = forces[...] - 0.5 * (flux[9 : 9 + count, :] - flux[7 : 7 + count, :])


def finish(sizes, table, packed, out, state):
    count = out.shape[0]
    values = table[...]
    row = lax.broadcasted_iota(jnp.int32, values.shape, 0)
    lane = lax.broadcasted_iota(jnp.int32, values.shape, 1)

    def pick(mask):
        kept = jnp.where(mask, values, -jnp.inf)
        return jnp.max(jnp.max(kept, axis=0, keepdims=True), axis=1, keepdims=True)

    ys, xs, zs, cs = sizes
    total = ys * xs * zs * cs
    spot = [lax.axis_index(name) for name in MACRO]
    here = ((spot[0] * xs + spot[1]) * zs + spot[2]) * cs + spot[3]
    prev_row, prev_low = group_spot(sizes, (here + total - 1) % total)
    next_row, next_low = group_spot(sizes, (here + 1) % total)
    fastest = pick((lane == 0) & (row % 2 == 0))
    prev_speed = pick((row == 2 * prev_row) & (lane == 2 + 2 * prev_low))
    next_speed = pick((row == 2 * next_row) & (lane == 1 + 2 * next_low))
    behind = table[pl.ds(2 * prev_row + 1, 1), :]
    ahead = table[pl.ds(2 * next_row + 1, 1), :]
    time_step = 0.8 / jnp.maximum(fastest, 1.0)
    state[8 : 8 + count, :] = packed[:count, :]
    state[7:8, :] = behind
    state[8 + count : 9 + count, :] = ahead
    u0, u1, u2 = (state[k : k + count, :] for k in (7, 8, 9))
    out[...] = u1 + time_step * (packed[count:, :] + 0.5 * fastest * ((u2 - u1) - (u1 - u0)))
    out[:1, :] = out[:1, :] + 0.5 * time_step * (prev_speed * behind)
    out[count - 1 :, :] = out[count - 1 :, :] - 0.5 * time_step * (next_speed * ahead)


def place(start, array, _, out, sem):
    replicas, points, _ = array.shape
    spot = pl.ds(pl.multiple_of((1 - lax.axis_index("micro")) * points, points), points)
    copy = pltpu.make_async_copy(array, out.at[pl.ds(start, replicas), spot, :], sem.at[0])
    copy.start()
    copy.wait()


def placed_in(array, start, out):
    return call(
        functools.partial(place, start),
        jax.ShapeDtypeStruct(out.shape, out.dtype),
        [array, out],
        specs=[VM, HBM],
        out_specs=HBM,
        scratch=[pltpu.SemaphoreType.DMA((1,))],
        aliases={1: 0},
    )


def swapped(value):
    return lax.ppermute(value, "micro", [(0, 1), (1, 0)])


def near_copy(value, low_z, core):
    count = lax.axis_size("macro_2")
    spots = [(z, c) for z in range(count) for c in range(2)]
    pairs = [(z * 2 + c, (z ^ low_z) * 2 + (c ^ core)) for z, c in spots]
    return lax.ppermute(value, ("macro_2", "macro_3"), pairs)


def starts(sizes):
    return [sum(sizes[:k]) for k in range(len(sizes))]


def shards(macro_state, micro_state, velocity, propagator, forcing_map, readout, speed_weights):
    f32, bf16 = jnp.float32, jnp.bfloat16
    count, fields = macro_state.shape
    half = micro_state.shape[2]
    points = count // 2
    micro = jnp.transpose(micro_state, (1, 0, 2))

    begin = starts(CHUNKS)
    chunks = [jax.ShapeDtypeStruct((size, points, half), bf16) for size in CHUNKS]
    first = call(
        functools.partial(cut_first, CHUNKS[0], points),
        jax.ShapeDtypeStruct((CHUNKS[0] * points + SHARE, half), bf16),
        [micro, propagator, forcing_map, readout],
        specs=[HBM] * 4,
        scratch=[
            pltpu.VMEM((2, 16, half), f32),
            pltpu.SemaphoreType.DMA((CHUNKS[0],)),
            pltpu.SemaphoreType.DMA((3,)),
        ],
        limit=FIRST_BYTES,
    )
    plan = tuple((at, False) for at in begin[1:])
    rest = call(
        functools.partial(cut_rest, plan),
        tuple(chunks[1:]),
        [micro, first],
        specs=[HBM, ANY],
        scratch=[pltpu.SemaphoreType.DMA((len(plan),))],
        limit=REST_BYTES,
    )
    arrived = []
    for value in [first, *rest]:
        arrived.append(swapped(value))
    share = arrived[0][CHUNKS[0] * points :]
    other = near_copy(share, 2, 0)
    share = jnp.stack([share, other])
    shares = [share]
    for z, c in ((0, 1), (1, 0), (1, 1)):
        shares.append(near_copy(share, z, c))
    weights = speed_weights.reshape(1, fields)
    speed_base = velocity.reshape(count // 128, 128)
    sums = jax.ShapeDtypeStruct((points, 2 * half), f32)
    matrix, forcing, far_readout = call(
        functools.partial(prepare, half),
        (jax.ShapeDtypeStruct((2 * half, 2 * half), bf16), sums, jax.ShapeDtypeStruct(readout.shape, f32)),
        [*shares, propagator, forcing_map, macro_state],
        scratch=[pltpu.VMEM(forcing_map.shape, f32)],
        flops=10**8,
    )
    out_type = jax.ShapeDtypeStruct(micro.shape, bf16)
    far_parts = []
    out = total = None
    for members in GROUPS:
        size_of_group = sum(CHUNKS[k] for u in members for k in UNITS[u])
        group, at = None, 0
        for u in members:
            parts, start = len(UNITS[u]), begin[UNITS[u][0]]
            size = sum(CHUNKS[k] for k in UNITS[u])
            whole = jax.ShapeDtypeStruct((size_of_group, points, half), bf16)
            ins = [micro, *(arrived[k] for k in UNITS[u]), matrix, forcing]
            specs, aliases = [HBM] + [VM] * (parts + 2), {}
            inner = out is not None
            if inner:
                aliases = {len(ins): 0, len(ins) + 1: 2}
                ins += [out, total]
                specs += [HBM, VM]
            if group is not None:
                aliases[len(ins)] = 1
                ins.append(group)
                specs.append(VM)
            scratch = [pltpu.VMEM((size * points, 2 * half), bf16)] * 2
            scratch += [pltpu.VMEM((size, points, half), bf16), pltpu.SemaphoreType.DMA((2,))]
            work = 2 * STEPS * size * points * (2 * half) ** 2
            if u < len(UNITS) - 1:
                out, group, total = call(
                    functools.partial(advance, start, at, parts, inner, group is not None),
                    (out_type, whole, sums),
                    ins,
                    specs=specs,
                    out_specs=(HBM, VM, VM),
                    scratch=scratch,
                    flops=work,
                    aliases=aliases,
                )
            else:
                aliases = {i: o for i, o in aliases.items() if o != 2}
                out, group, message, note = call(
                    functools.partial(advance_last, start, at, parts, group is not None),
                    (
                        out_type,
                        whole,
                        jax.ShapeDtypeStruct((points + 48, 128), bf16),
                        jax.ShapeDtypeStruct((8, 128), f32),
                    ),
                    [*ins, readout, far_readout, weights, speed_base, macro_state],
                    specs=specs + [VM] * 5,
                    out_specs=(HBM, VM, VM, VM),
                    scratch=[pltpu.VMEM(sums.shape, f32), *scratch],
                    flops=work,
                    aliases=aliases,
                )
            at += size
        far_parts.append(group)

    across = swapped(message)
    beside = lax.ppermute(note, "macro_1", [(0, 1), (1, 0)])
    both = lax.ppermute(note, ("macro_1", "micro"), [(k, 3 - k) for k in range(4)])
    returned = []
    for value in far_parts:
        returned.append(swapped(value))
    group = lax.axis_size(GROUP)
    sizes = tuple(lax.axis_size(name) for name in MACRO)
    rows = call(
        functools.partial(combine, sizes), jax.ShapeDtypeStruct((2 * group, 128), f32), [note, across, beside, both]
    )
    table = lax.all_to_all(rows.reshape(group, 2, 128), GROUP, split_axis=0, concat_axis=0, tiled=True)
    table = table.reshape(2 * group, 128)
    padded = pltpu.VMEM((count + 16, fields), f32)
    packed = call(
        before_finish,
        jax.ShapeDtypeStruct((2 * count, fields), f32),
        [message, across, macro_state, speed_base, weights],
        scratch=[pltpu.VMEM((count, fields), f32), padded],
    )
    macro_next = call(
        functools.partial(finish, sizes), jax.ShapeDtypeStruct((count, fields), f32), [table, packed], scratch=[padded]
    )
    for members, value in zip(GROUPS, returned):
        out = placed_in(value, begin[UNITS[members[0]][0]], out)
    return macro_next, jnp.transpose(out, (1, 0, 2))


def solution(mesh):
    torus = Mesh(
        mesh.devices.reshape(4, 2, 8, 2, mesh.shape["micro"]),
        ("macro_0", "macro_1", "macro_2", "macro_3", "micro"),
    )
    placed = (
        P(MACRO, None),
        P(MACRO, None, "micro"),
        P(MACRO),
        P(None, "micro"),
        P(None, "micro"),
        P(None, "micro"),
        P(),
    )
    return jax.shard_map(
        shards,
        mesh=torus,
        in_specs=placed,
        out_specs=(P(MACRO, None), P(MACRO, None, "micro")),
        check_vma=False,
    )
```

```python
import functools

import jax
import jax.numpy as jnp
from jax import lax
from jax.experimental import pallas as pl
from jax.experimental.pallas import tpu as pltpu
from jax.sharding import Mesh
from jax.sharding import PartitionSpec as P


S = 12
STEPS = 4
MACRO = ("macro_0", "macro_1", "macro_2", "macro_3")
GROUP = ("macro_0", "macro_2", "macro_3")
CHUNKS = (1, 2, 5, 3, 1)
UNITS = ((0, 1), (2,), (3,), (4,))
GROUPS = ((0,), (1, 2, 3))
SHARE = 128
HIGHEST = lax.Precision.HIGHEST
VM = pl.BlockSpec(memory_space=pltpu.VMEM)
ANY = pl.BlockSpec(memory_space=pl.ANY)
HBM = pl.BlockSpec(memory_space=pltpu.HBM)
VMEM_BYTES = 6 * 2**20
FIRST_BYTES = 66_800_000
REST_BYTES = 60_500_000


def call(body, outs, ins, specs=None, scratch=(), flops=0, aliases=None, out_specs=None, limit=None):
    size = sum(a.size * a.dtype.itemsize for a in ins)
    return pl.pallas_call(
        body,
        out_shape=outs,
        in_specs=specs or [VM] * len(ins),
        out_specs=out_specs or jax.tree.map(lambda _: VM, outs),
        scratch_shapes=list(scratch),
        input_output_aliases=aliases or {},
        compiler_params=pltpu.CompilerParams(vmem_limit_bytes=limit or VMEM_BYTES),
        cost_estimate=pl.CostEstimate(flops=flops, bytes_accessed=size, transcendentals=0),
    )(*ins)


def f32dot(a, b, contract=((1,), (0,))):
    return lax.dot_general(a, b, (contract, ((), ())), precision=HIGHEST, preferred_element_type=jnp.float32)


def eighth():
    return (lax.axis_index("macro_2") % 4) * 2 + lax.axis_index("macro_3")


def slice_copies(plan, micro, outs, sems):
    me = lax.axis_index("micro")
    copies = []
    for k, ((start, mine), out) in enumerate(zip(plan, outs)):
        replicas, points, _ = out.shape
        at = (me if mine else 1 - me) * points
        where = micro.at[pl.ds(start, replicas), pl.ds(pl.multiple_of(at, points), points), :]
        copies.append(pltpu.make_async_copy(where, out, sems.at[k]))
    return copies


def cut_first(replicas, points, micro, prop, fmap, readout, out, maps, sems, more):
    e = eighth()
    base = replicas * points
    small = pl.ds(pl.multiple_of(e * 16, 16), 16)
    spot = pl.ds(pl.multiple_of((1 - lax.axis_index("micro")) * points, points), points)
    copies = [
        pltpu.make_async_copy(micro.at[k, spot, :], out.at[pl.ds(k * points, points), :], sems.at[k])
        for k in range(replicas)
    ]
    copies += [
        pltpu.make_async_copy(fmap.at[small, :], maps.at[0], more.at[0]),
        pltpu.make_async_copy(readout.at[small, :], maps.at[1], more.at[1]),
        pltpu.make_async_copy(
            prop.at[pl.ds(pl.multiple_of(e * 64, 64), 64), :], out.at[pl.ds(base, 64), :], more.at[2]
        ),
    ]
    for copy in copies:
        copy.start()
    for copy in copies:
        copy.wait()
    for k in range(2):
        rows = maps[k]
        high = rows.astype(jnp.bfloat16)
        at = base + 64 + 32 * k
        out[at : at + 16, :] = high
        out[at + 16 : at + 32, :] = (rows - high.astype(jnp.float32)).astype(jnp.bfloat16)


def cut_rest(plan, micro, _, *refs):
    copies = slice_copies(plan, micro, refs[:-1], refs[-1])
    for copy in copies:
        copy.start()
    for copy in copies:
        copy.wait()


def prepare(half, s0, s1, s2, s3, prop, fmap, macro, matrix_out, forcing_out, readout_out, far_map):
    me, e = lax.axis_index("micro"), eighth()
    points = forcing_out.shape[0]
    core, low_z, mid_z = e % 2, (e // 2) % 2, e // 4
    for k, pair in enumerate((s0, s1, s2, s3)):
        c = core if k % 2 == 0 else 1 - core
        z = low_z if k < 2 else 1 - low_z
        for t in range(2):
            share = pair.at[t]
            y = mid_z if t == 0 else 1 - mid_z
            y_row = (y + me) % 2
            spot = pl.ds(pl.multiple_of((y_row * 4 + z * 2 + c) * 64, 64), 64)
            matrix_out[spot, half:] = share[:64, :]
            at = pl.ds(pl.multiple_of((y * 4 + z * 2 + c) * 16, 16), 16)
            far_map[at, :] = share[64:80, :].astype(jnp.float32) + share[80:96, :].astype(jnp.float32)
            readout_out[at, :] = share[96:112, :].astype(jnp.float32) + share[112:128, :].astype(jnp.float32)
    matrix_out[:half, :half] = prop[pl.ds(pl.multiple_of(me * half, half), half), :]
    matrix_out[half:, :half] = prop[pl.ds(pl.multiple_of((1 - me) * half, half), half), :]
    mine = macro[pl.ds(pl.multiple_of(me * points, points), points), :]
    forcing_out[:, :half] = jnp.tanh(f32dot(mine, fmap[...]))
    forcing_out[:, half:] = jnp.tanh(f32dot(mine, far_map[...]))


def steps_of(start, at, micro, fars, matrix, forcing, total_in, out, far_out, total_out, now, after, keep, sem):
    points, half = far_out.shape[1:]
    replicas = keep.shape[0]
    rows = replicas * points
    spot = pl.ds(pl.multiple_of(lax.axis_index("micro") * points, points), points)
    near = pltpu.make_async_copy(micro.at[pl.ds(start, replicas), spot, :], keep, sem.at[1])
    near.start()
    row = 0
    for far in fars:
        count = far.shape[0] * points if len(far.shape) == 3 else far.shape[0] - SHARE
        now[row : row + count, half:] = far[:count, :] if len(far.shape) == 2 else far[...].reshape(count, half)
        row += count
    near.wait()
    now[:, :half] = keep[...].reshape(rows, half)
    source, target = now, after
    copy = pltpu.make_async_copy(keep, out.at[pl.ds(start, replicas), spot, :], sem.at[0])
    for step in range(STEPS):
        for side in range(2):
            cols = slice(side * half, side * half + half)
            summed = jnp.dot(source[...], matrix[:, cols], preferred_element_type=jnp.float32)
            state = (summed.reshape(replicas, points, half) + forcing[:, cols][None]).astype(jnp.bfloat16)
            share = jnp.sum(jnp.tanh(state.astype(jnp.float32)), axis=0)
            if step > 0:
                share = total_out[:, cols] + share
            elif total_in is not None:
                share = total_in[:, cols] + share
            total_out[:, cols] = share
            if step < STEPS - 1:
                target[:, cols] = state.reshape(rows, half)
            elif side == 0:
                keep[...] = state
                copy.start()
            else:
                far_out[at : at + replicas] = state
        source, target = target, source
    return copy


def advance(start, at, parts, inner, has_group, micro, *refs):
    fars, (matrix, forcing), refs = refs[:parts], refs[parts : parts + 2], refs[parts + 2 :]
    total_in = refs[1] if inner else None
    out, far_out, total, now, after, keep, sem = refs[2 * inner + has_group :]
    copy = steps_of(start, at, micro, fars, matrix, forcing, total_in, out, far_out, total, now, after, keep, sem)
    copy.wait()


def spread(row):
    return jnp.broadcast_to(row, (row.shape[1], row.shape[1])).T


def base_speeds(velocity, start, count):
    return jnp.concatenate([spread(velocity[pl.ds(start + k, 1), :]) for k in range(count)], axis=0)


def advance_last(start, at, parts, has_group, micro, *refs):
    fars, (matrix, forcing), refs = refs[:parts], refs[parts : parts + 2], refs[parts + 3 :]
    total_in, refs = refs[0], refs[1 + has_group :]
    readout, far_readout, weights, velocity, macro, out, far_out, message, note = refs[:9]
    total, now, after, keep, sem = refs[9:]
    copy = steps_of(start, at, micro, fars, matrix, forcing, total_in, out, far_out, total, now, after, keep, sem)
    points, half = far_out.shape[1:]
    me = lax.axis_index("micro")
    averaged = total[...] / (STEPS * S)
    forces = f32dot(averaged[:, :half], readout[...], ((1,), (1,)))
    forces = forces + f32dot(averaged[:, half:], far_readout[...], ((1,), (1,)))
    forces = forces.astype(jnp.bfloat16)
    message[:points, :] = forces
    drive = f32dot(forces.astype(jnp.float32), spread(weights[...]))
    blocks = points // 128
    speeds = base_speeds(velocity, me * blocks, blocks) * (1.5 + jnp.tanh(drive))
    row = lax.broadcasted_iota(jnp.int32, (8, speeds.shape[1]), 0)
    top = jnp.max(speeds, axis=0, keepdims=True)
    values = jnp.where(row == 0, top, jnp.where(row == 1, speeds[:1, :], speeds[points - 1 :, :]))
    count = macro.shape[0]
    note[...] = jnp.where(row == 3, macro[:1, :], jnp.where(row == 4, macro[count - 1 :, :], values))
    row = lax.broadcasted_iota(jnp.int32, (16, speeds.shape[1]), 0)
    rest = jnp.where(row % 3 == 0, top, jnp.where(row % 3 == 1, speeds[:1, :], speeds[points - 1 :, :]))
    parts = []
    for _ in range(3):
        parts.append(rest.astype(jnp.bfloat16).astype(jnp.float32))
        rest = rest - parts[-1]
    message[points:, :] = jnp.where(row < 3, parts[0], jnp.where(row < 6, parts[1], parts[2])).astype(jnp.bfloat16)
    copy.wait()


def group_spot(sizes, index):
    _, xs, zs, cs = sizes
    y = index // (cs * zs * xs)
    return (y * zs + (index // cs) % zs) * cs + index % cs, (index // (cs * zs)) % xs


def combine(sizes, own, across, beside, both, out):
    ys, xs, zs, cs = sizes
    me = lax.axis_index("micro")
    y, low, z, core = (lax.axis_index(name) for name in MACRO)
    first, zero = me == 0, low == 0
    far = across[across.shape[0] - 16 :, :].astype(jnp.float32)
    a, c, d = ([ref[k : k + 1, :] for k in range(3)] for ref in (own, beside, both))
    b = [far[k : k + 1, :] + far[k + 3 : k + 4, :] + far[k + 6 : k + 7, :] for k in range(3)]
    top = jnp.maximum(jnp.maximum(a[0], b[0]), jnp.maximum(c[0], d[0]))
    mine = (jnp.where(first, a[1], b[1]), jnp.where(first, b[2], a[2]))
    other = (jnp.where(first, c[1], d[1]), jnp.where(first, d[2], c[2]))
    block0 = [jnp.where(zero, x, v) for x, v in zip(mine, other)]
    block1 = [jnp.where(zero, v, x) for x, v in zip(mine, other)]
    lane = lax.broadcasted_iota(jnp.int32, top.shape, 1)
    value = top
    for k, v in enumerate(block0 + block1):
        value = jnp.where(lane == k + 1, v, value)
    total = ys * xs * zs * cs
    up = (z == zs - 1) & (core == cs - 1)
    down = (z == 0) & (core == 0)
    after_low = jnp.where(up, 1 - low, low)
    before_low = jnp.where(down, 1 - low, low)
    after_spot, _ = group_spot(sizes, (((y * xs + after_low) * zs + z) * cs + core + 1) % total)
    before_spot, _ = group_spot(sizes, (((y * xs + before_low) * zs + z) * cs + core + total - 1) % total)
    last_state = jnp.where(up, beside[4:5, :], own[4:5, :])
    first_state = jnp.where(down, beside[3:4, :], own[3:4, :])
    row = lax.broadcasted_iota(jnp.int32, out.shape, 0)
    rows = jnp.where(row % 2 == 0, value, 0.0)
    rows = jnp.where(row == 2 * after_spot + 1, last_state, rows)
    out[...] = jnp.where(row == 2 * before_spot + 1, first_state, rows)


def before_finish(own, across, macro, velocity, weights, packed, forces, flux):
    me = lax.axis_index("micro")
    points = own.shape[0] - 16
    count = macro.shape[0]
    forces[pl.ds(pl.multiple_of(me * points, points), points), :] = own[:points, :].astype(jnp.float32)
    forces[pl.ds(pl.multiple_of((1 - me) * points, points), points), :] = across[:points, :].astype(jnp.float32)
    flux[:8, :] = jnp.zeros((8, flux.shape[1]), jnp.float32)
    flux[8 + count :, :] = jnp.zeros((8, flux.shape[1]), jnp.float32)
    base = base_speeds(velocity, 0, count // 128)
    flux[8 : 8 + count, :] = base * (1.5 + jnp.tanh(f32dot(forces[...], spread(weights[...])))) * macro[...]
    packed[:count, :] = macro[...]
    packed[count:, :] = forces[...] - 0.5 * (flux[9 : 9 + count, :] - flux[7 : 7 + count, :])


def finish(sizes, table, packed, out, state):
    count = out.shape[0]
    values = table[...]
    row = lax.broadcasted_iota(jnp.int32, values.shape, 0)
    lane = lax.broadcasted_iota(jnp.int32, values.shape, 1)

    def pick(mask):
        kept = jnp.where(mask, values, -jnp.inf)
        return jnp.max(jnp.max(kept, axis=0, keepdims=True), axis=1, keepdims=True)

    ys, xs, zs, cs = sizes
    total = ys * xs * zs * cs
    spot = [lax.axis_index(name) for name in MACRO]
    here = ((spot[0] * xs + spot[1]) * zs + spot[2]) * cs + spot[3]
    prev_row, prev_low = group_spot(sizes, (here + total - 1) % total)
    next_row, next_low = group_spot(sizes, (here + 1) % total)
    fastest = pick((lane == 0) & (row % 2 == 0))
    prev_speed = pick((row == 2 * prev_row) & (lane == 2 + 2 * prev_low))
    next_speed = pick((row == 2 * next_row) & (lane == 1 + 2 * next_low))
    behind = table[pl.ds(2 * prev_row + 1, 1), :]
    ahead = table[pl.ds(2 * next_row + 1, 1), :]
    time_step = 0.8 / jnp.maximum(fastest, 1.0)
    state[8 : 8 + count, :] = packed[:count, :]
    state[7:8, :] = behind
    state[8 + count : 9 + count, :] = ahead
    u0, u1, u2 = (state[k : k + count, :] for k in (7, 8, 9))
    out[...] = u1 + time_step * (packed[count:, :] + 0.5 * fastest * ((u2 - u1) - (u1 - u0)))
    out[:1, :] = out[:1, :] + 0.5 * time_step * (prev_speed * behind)
    out[count - 1 :, :] = out[count - 1 :, :] - 0.5 * time_step * (next_speed * ahead)


def place(start, array, _, out, sems):
    replicas, points, _ = array.shape
    spot = pl.ds(pl.multiple_of((1 - lax.axis_index("micro")) * points, points), points)
    copies = [
        pltpu.make_async_copy(array.at[k], out.at[start + k, spot, :], sems.at[k]) for k in range(replicas)
    ]
    for copy in copies:
        copy.start()
    for copy in copies:
        copy.wait()


def placed_in(array, start, out):
    return call(
        functools.partial(place, start),
        jax.ShapeDtypeStruct(out.shape, out.dtype),
        [array, out],
        specs=[VM, HBM],
        out_specs=HBM,
        scratch=[pltpu.SemaphoreType.DMA((array.shape[0],))],
        aliases={1: 0},
    )


def swapped(value):
    return lax.ppermute(value, "micro", [(0, 1), (1, 0)])


def near_copy(value, low_z, core):
    count = lax.axis_size("macro_2")
    spots = [(z, c) for z in range(count) for c in range(2)]
    pairs = [(z * 2 + c, (z ^ low_z) * 2 + (c ^ core)) for z, c in spots]
    return lax.ppermute(value, ("macro_2", "macro_3"), pairs)


def starts(sizes):
    return [sum(sizes[:k]) for k in range(len(sizes))]


def shards(macro_state, micro_state, velocity, propagator, forcing_map, readout, speed_weights):
    f32, bf16 = jnp.float32, jnp.bfloat16
    count, fields = macro_state.shape
    half = micro_state.shape[2]
    points = count // 2
    micro = jnp.transpose(micro_state, (1, 0, 2))

    begin = starts(CHUNKS)
    chunks = [jax.ShapeDtypeStruct((size, points, half), bf16) for size in CHUNKS]
    first = call(
        functools.partial(cut_first, CHUNKS[0], points),
        jax.ShapeDtypeStruct((CHUNKS[0] * points + SHARE, half), bf16),
        [micro, propagator, forcing_map, readout],
        specs=[HBM] * 4,
        scratch=[
            pltpu.VMEM((2, 16, half), f32),
            pltpu.SemaphoreType.DMA((CHUNKS[0],)),
            pltpu.SemaphoreType.DMA((3,)),
        ],
        limit=FIRST_BYTES,
    )
    plan = tuple((at, False) for at in begin[1:])
    rest = call(
        functools.partial(cut_rest, plan),
        tuple(chunks[1:]),
        [micro, first],
        specs=[HBM, ANY],
        scratch=[pltpu.SemaphoreType.DMA((len(plan),))],
        limit=REST_BYTES,
    )
    arrived = []
    for value in [first, *rest]:
        arrived.append(swapped(value))
    share = arrived[0][CHUNKS[0] * points :]
    other = near_copy(share, 2, 0)
    share = jnp.stack([share, other])
    shares = [share]
    for z, c in ((0, 1), (1, 0), (1, 1)):
        shares.append(near_copy(share, z, c))
    weights = speed_weights.reshape(1, fields)
    speed_base = velocity.reshape(count // 128, 128)
    sums = jax.ShapeDtypeStruct((points, 2 * half), f32)
    matrix, forcing, far_readout = call(
        functools.partial(prepare, half),
        (jax.ShapeDtypeStruct((2 * half, 2 * half), bf16), sums, jax.ShapeDtypeStruct(readout.shape, f32)),
        [*shares, propagator, forcing_map, macro_state],
        scratch=[pltpu.VMEM(forcing_map.shape, f32)],
        flops=10**8,
    )
    out_type = jax.ShapeDtypeStruct(micro.shape, bf16)
    far_parts = []
    out = total = None
    for members in GROUPS:
        size_of_group = sum(CHUNKS[k] for u in members for k in UNITS[u])
        group, at = None, 0
        for u in members:
            parts, start = len(UNITS[u]), begin[UNITS[u][0]]
            size = sum(CHUNKS[k] for k in UNITS[u])
            whole = jax.ShapeDtypeStruct((size_of_group, points, half), bf16)
            ins = [micro, *(arrived[k] for k in UNITS[u]), matrix, forcing]
            specs, aliases = [HBM] + [VM] * (parts + 2), {}
            inner = out is not None
            if inner:
                aliases = {len(ins): 0, len(ins) + 1: 2}
                ins += [out, total]
                specs += [HBM, VM]
            if group is not None:
                aliases[len(ins)] = 1
                ins.append(group)
                specs.append(VM)
            scratch = [pltpu.VMEM((size * points, 2 * half), bf16)] * 2
            scratch += [pltpu.VMEM((size, points, half), bf16), pltpu.SemaphoreType.DMA((2,))]
            work = 2 * STEPS * size * points * (2 * half) ** 2
            if u < len(UNITS) - 1:
                out, group, total = call(
                    functools.partial(advance, start, at, parts, inner, group is not None),
                    (out_type, whole, sums),
                    ins,
                    specs=specs,
                    out_specs=(HBM, VM, VM),
                    scratch=scratch,
                    flops=work,
                    aliases=aliases,
                )
            else:
                aliases = {i: o for i, o in aliases.items() if o != 2}
                out, group, message, note = call(
                    functools.partial(advance_last, start, at, parts, group is not None),
                    (
                        out_type,
                        whole,
                        jax.ShapeDtypeStruct((points + 16, 128), bf16),
                        jax.ShapeDtypeStruct((8, 128), f32),
                    ),
                    [*ins, readout, far_readout, weights, speed_base, macro_state],
                    specs=specs + [VM] * 5,
                    out_specs=(HBM, VM, VM, VM),
                    scratch=[pltpu.VMEM(sums.shape, f32), *scratch],
                    flops=work,
                    aliases=aliases,
                )
            at += size
        far_parts.append(group)

    across = swapped(message)
    beside = lax.ppermute(note, "macro_1", [(0, 1), (1, 0)])
    both = lax.ppermute(note, ("macro_1", "micro"), [(k, 3 - k) for k in range(4)])
    returned = []
    for value in far_parts:
        returned.append(swapped(value))
    group = lax.axis_size(GROUP)
    sizes = tuple(lax.axis_size(name) for name in MACRO)
    rows = call(
        functools.partial(combine, sizes), jax.ShapeDtypeStruct((2 * group, 128), f32), [note, across, beside, both]
    )
    table = lax.all_to_all(rows.reshape(group, 2, 128), GROUP, split_axis=0, concat_axis=0, tiled=True)
    table = table.reshape(2 * group, 128)
    padded = pltpu.VMEM((count + 16, fields), f32)
    packed = call(
        before_finish,
        jax.ShapeDtypeStruct((2 * count, fields), f32),
        [message, across, macro_state, speed_base, weights],
        scratch=[pltpu.VMEM((count, fields), f32), padded],
    )
    macro_next = call(
        functools.partial(finish, sizes), jax.ShapeDtypeStruct((count, fields), f32), [table, packed], scratch=[padded]
    )
    for members, value in zip(GROUPS, returned):
        out = placed_in(value, begin[UNITS[members[0]][0]], out)
    return macro_next, jnp.transpose(out, (1, 0, 2))


def solution(mesh):
    torus = Mesh(
        mesh.devices.reshape(4, 2, 8, 2, mesh.shape["micro"]),
        ("macro_0", "macro_1", "macro_2", "macro_3", "micro"),
    )
    placed = (
        P(MACRO, None),
        P(MACRO, None, "micro"),
        P(MACRO),
        P(None, "micro"),
        P(None, "micro"),
        P(None, "micro"),
        P(),
    )
    return jax.shard_map(
        shards,
        mesh=torus,
        in_specs=placed,
        out_specs=(P(MACRO, None), P(MACRO, None, "micro")),
        check_vma=False,
    )
```
